32 devices in a mesh: band: 4 (over y, core), grid: 8 (over z, x).
Axes of the slice: x: 2, y: 2, z: 4, core: 2. Of those that a mesh axis runs over, the one named last changes fastest.
Arguments:
- orbitals: bfloat16 [64, 2, 16, 128, 128], P('band', None, 'grid'), may hold values from -1.5 to 1.5
- occupations: float32 [64], P('band'), may hold values from 0.2 to 2
Outputs:
- current: float32 [3, 16, 128, 128], P(None, 'grid', 'band')
The draws below stay inside these ranges and needn't reach their ends.
All inputs are finite; a program needn't handle non-finite values.
Results may differ from the reference program's by a relative error of at most 0.0003.
Values may be sent and summed in bfloat16 or wider, within the bound.
No kernel may reach another device: no remote copies, remote signals or barrier semaphores. Data moves between devices by JAX's collectives and lax.ppermute only.
A program may use at most 64 MiB of HBM per device.

```python
import jax
import jax.numpy as jnp
from jax import lax

NX = 128
NY = 128
BANDS = 64
NZ = 16


def block_scale(key, extent, cuts, smallest, top_value):
    def one(axis_at, parts):
        steps = jax.random.uniform(jax.random.fold_in(jax.random.fold_in(key, 6), axis_at), (parts,), jnp.float32, smallest / len(cuts), top_value / len(cuts))
        return jnp.repeat(jnp.exp(steps), extent[axis_at] // parts).reshape((-1,) + (1,) * (len(extent) - axis_at - 1))

    level = one(*cuts[0])
    for cut in cuts[1:]:
        level = level * one(*cut)
    return level


def normal_values(key, shape, width, reach, pieces=(), held_as=jnp.bfloat16):
    entries = width * jax.random.normal(key, shape, jnp.float32)
    if pieces:
        entries = entries * block_scale(key, shape, pieces, -0.22, 0.18)
    return jnp.clip(entries, -reach, reach).astype(held_as)


def setup_inputs(seed: int = 0) -> dict:
    splits = jax.random.split(jax.random.key(seed), 3)
    return {
        "orbitals": normal_values(splits[0], (BANDS, 2, NZ, NX, NY), 0.25, 1.5, ((0, 4), (2, 8))),
        "occupations": jnp.clip(0.2 + 1.8 * jax.random.uniform(splits[1], (BANDS,), jnp.float32) ** block_scale(splits[1], (BANDS,), ((0, 4),), -0.2, 0.2), 0.2, 2.0),
    }


def derivative(values, direction):
    forward = jnp.roll(values, -1, direction) - jnp.roll(values, 1, direction)
    farther = jnp.roll(values, -2, direction) - jnp.roll(values, 2, direction)
    return (8.0 * forward - farther) / 12.0


def reference(orbitals, occupations):
    def advance(summed, item):
        orbital, weight = item
        real_part = orbital[0].astype(jnp.float32)
        imag_part = orbital[1].astype(jnp.float32)
        components = jnp.stack([real_part * derivative(imag_part, direction) - imag_part * derivative(real_part, direction) for direction in range(3)])
        return summed + weight * components, None

    initial = jnp.zeros((3, NZ, NX, NY), jnp.float32)
    summed, _ = lax.scan(advance, initial, (orbitals, occupations))
    return summed
```

```python
import functools

import jax
import jax.numpy as jnp
import numpy as np
from jax import lax
from jax.experimental import pallas as pl
from jax.experimental.pallas import tpu as pltpu
from jax.sharding import PartitionSpec as P


def stencil(cells):
    eye = np.eye(cells, dtype=np.float32)
    near = np.roll(eye, 1, 0) - np.roll(eye, -1, 0)
    far = np.roll(eye, 2, 0) - np.roll(eye, -2, 0)
    return jnp.asarray(8.0 * near - far, jnp.bfloat16)


def lateral_kernel(weights, block, across, along, out, total):
    step = pl.program_id(0)

    @pl.when(step == 0)
    def _():
        total[...] = jnp.zeros_like(total)

    weight = weights[step]
    fields = []
    for plane in range(2):
        re16 = block[0, 0, plane]
        im16 = block[0, 1, plane]
        re = weight * re16.astype(jnp.float32)
        im = weight * im16.astype(jnp.float32)
        fields.append((re, im, re16, im16))
        dot = functools.partial(jnp.dot, preferred_element_type=jnp.float32)
        total[1 + plane] += re * dot(across[...], im16) - im * dot(across[...], re16)
        total[3 + plane] += re * dot(im16, along[...]) - im * dot(re16, along[...])
    (re, im, _, _), (_, _, re_up, im_up) = fields
    total[0] += 8.0 * (re * im_up.astype(jnp.float32) - im * re_up.astype(jnp.float32))

    @pl.when(step == pl.num_programs(0) - 1)
    def _():
        rows = out.shape[3]
        for core in range(2):
            for half in range(2):
                at = (2 * half + core) * rows
                out[core, half] = total[:, at : at + rows] * (1.0 / 12.0)


def lateral(orbitals, weights):
    bands, parts, planes, nx, ny = orbitals.shape
    return pl.pallas_call(
        lateral_kernel,
        grid=(bands,),
        in_specs=[
            pl.BlockSpec(memory_space=pltpu.SMEM),
            pl.BlockSpec((1, parts, planes, nx, ny), lambda n: (n, 0, 0, 0, 0)),
            pl.BlockSpec((nx, nx), lambda n: (0, 0)),
            pl.BlockSpec((ny, ny), lambda n: (0, 0)),
        ],
        out_specs=pl.BlockSpec((2, 2, 5, nx // 4, ny), lambda n: (0, 0, 0, 0, 0)),
        out_shape=jax.ShapeDtypeStruct((2, 2, 5, nx // 4, ny), jnp.float32),
        scratch_shapes=[pltpu.VMEM((5, nx, ny), jnp.float32)],
        name="lateral",
    )(weights, orbitals, stencil(nx).T, stencil(ny))


def crossing(weight_sets, first_sets, second_sets, odd):
    rows, lanes = first_sets[0].shape[-2:]
    zero = jnp.zeros((rows, lanes), jnp.float32)
    sums = (zero, zero, zero)
    for weights, first, second in zip(weight_sets, first_sets, second_sets):

        def advance(n, sums):
            def pair(lower, upper):
                re, im = (weights[n] * first[n, part, lower].astype(jnp.float32) for part in range(2))
                re_up, im_up = (second[n, part, upper].astype(jnp.float32) for part in range(2))
                return re * im_up - im * re_up

            return (
                sums[0] + pair(0, 0),
                sums[1] + pair(1, 1),
                sums[2] + pair(1 - odd, odd),
            )

        sums = lax.fori_loop(0, first.shape[0], advance, sums, unroll=2)
    sign = (1 - 2 * odd).astype(jnp.float32) * (1.0 / 12.0)
    return sign * sums[0], sign * sums[1], (8.0 * sign) * sums[2]


def inner_kernel(flags, w1, w2, own1, own2, side1, side2, own_out, side_out):
    odd = flags[0]
    low, high, mid = crossing((w1, w2), (own1, own2), (side1, side2), odd)
    up = jnp.where(odd == 1, 1.0, 0.0)
    own_out[0] = up * mid - low
    own_out[1] = (1.0 - up) * mid - high
    side_out[0] = (1.0 - up) * mid - low
    side_out[1] = up * mid - high


def outer_kernel(flags, w1, w2, side1, side2, far1, far2, own_in, side_in, kept, near, middle, distant):
    odd = flags[0]
    corner = flags[1]
    low, high, mid = crossing((w1, w2), (side1, side2), (far1, far2), odd)
    up = jnp.where(odd == 1, 1.0, 0.0)
    own = own_in[...]
    side = side_in[...] + jnp.stack([up * mid - low, (1.0 - up) * mid - high])
    far = jnp.stack([(1.0 - up) * mid - low, up * mid - high])
    here = corner == 1
    kept[...] = jnp.where(here, own, 0.0)
    near[...] = jnp.where(here, side, own)
    middle[...] = jnp.where(here, far, side)
    distant[...] = far


def call(kernel, scalars, arrays, outs):
    smem = pl.BlockSpec(memory_space=pltpu.SMEM)
    vmem = pl.BlockSpec(memory_space=pltpu.VMEM)
    shape = arrays[0].shape
    out = jax.ShapeDtypeStruct((2,) + shape[-2:], jnp.float32)
    return pl.pallas_call(
        kernel,
        in_specs=[smem] * len(scalars) + [vmem] * len(arrays),
        out_specs=[vmem] * outs,
        out_shape=[out] * outs,
        name=kernel.__name__,
    )(*scalars, *arrays)


def per_device(orbitals, occupations):
    slabs = lax.axis_size("grid")
    groups = lax.axis_size("band")
    assert groups == 4 and slabs % 2 == 0 and orbitals.shape[2] == 2
    slab = lax.axis_index("grid")
    group = lax.axis_index("band")
    odd = slab % 2
    core = group % 2
    half = group // 2
    corner = (half == odd).astype(jnp.int32)
    flags = jnp.stack([odd, corner]).astype(jnp.int32)
    quarter = orbitals.shape[3] // 4

    def beyond(g):
        return (g + 2) % slabs if g % 2 else (g - 2) % slabs

    def home(g):
        return (g - 2) % slabs if g % 2 else (g + 2) % slabs

    def route(value, target):
        pairs = []
        for b in range(groups):
            for g in range(slabs):
                goal = target(b, g)
                if goal is not None:
                    pairs.append((b * slabs + g, goal[0] * slabs + goal[1]))
        return lax.ppermute(value, ("band", "grid"), pairs)

    def rows(index):
        return lax.dynamic_slice_in_dim(orbitals, index * quarter, quarter, 3)

    own = rows(2 * odd + core)
    own_across = rows(2 * odd + 1 - core)
    side = rows(2 * (1 - odd) + core)
    side_across = rows(2 * (1 - odd) + 1 - core)

    w2 = route(occupations, lambda b, g: (b ^ 1, g))
    far1 = route(own, lambda b, g: (b, beyond(g)))
    side1 = route(side, lambda b, g: (b, g ^ 1))
    far2 = route(own_across, lambda b, g: (b ^ 1, beyond(g)))
    side2 = route(side_across, lambda b, g: (b ^ 1, g ^ 1))
    own2 = route(own_across, lambda b, g: (b ^ 1, g))

    flat = lateral(orbitals, occupations)
    flat = flat[core] + route(flat[1 - core], lambda b, g: (b ^ 1, g))
    flat = flat[half] + route(flat[1 - half], lambda b, g: (b ^ 2, g))

    weights = (occupations, w2)
    own_part, side_part = call(inner_kernel, (flags, *weights), (own, own2, side1, side2), 2)
    kept, near, middle, distant = call(
        outer_kernel,
        (flags, *weights),
        (side1, side2, far1, far2, own_part, side_part),
        4,
    )

    def is_corner(b, g):
        return b // 2 == g % 2

    got = route(distant, lambda b, g: None if is_corner(b, g) else (b ^ 2, home(g)))
    got_middle = route(
        middle, lambda b, g: (b, home(g)) if is_corner(b, g) else (b ^ 2, g ^ 1)
    )
    got_near = route(near, lambda b, g: (b, g ^ 1) if is_corner(b, g) else (b ^ 2, g))
    depth = flat[0][None] + kept + got_near + got_middle + got
    return jnp.stack([depth, flat[1:3], flat[3:5]])


def solution(mesh):
    placed = (P("band", None, "grid", None, None), P("band"))
    return jax.shard_map(
        per_device,
        mesh=mesh,
        in_specs=placed,
        out_specs=P(None, "grid", "band", None),
        check_vma=False,
    )
```

```python
import functools

import jax
import jax.numpy as jnp
import numpy as np
from jax import lax
from jax.experimental import pallas as pl
from jax.experimental.pallas import tpu as pltpu
from jax.sharding import PartitionSpec as P


def stencil(cells):
    eye = np.eye(cells, dtype=np.float32)
    near = np.roll(eye, 1, 0) - np.roll(eye, -1, 0)
    far = np.roll(eye, 2, 0) - np.roll(eye, -2, 0)
    return jnp.asarray(8.0 * near - far, jnp.bfloat16)


def lateral_kernel(weights, block, across, along, out, total):
    step = pl.program_id(0)

    @pl.when(step == 0)
    def _():
        total[...] = jnp.zeros_like(total)

    weight = weights[step]
    fields = []
    for plane in range(2):
        re16 = block[0, 0, plane]
        im16 = block[0, 1, plane]
        re = weight * re16.astype(jnp.float32)
        im = weight * im16.astype(jnp.float32)
        fields.append((re, im, re16, im16))
        dot = functools.partial(jnp.dot, preferred_element_type=jnp.float32)
        total[1 + plane] += re * dot(across[...], im16) - im * dot(across[...], re16)
        total[3 + plane] += re * dot(im16, along[...]) - im * dot(re16, along[...])
    (re, im, _, _), (_, _, re_up, im_up) = fields
    total[0] += 8.0 * (re * im_up.astype(jnp.float32) - im * re_up.astype(jnp.float32))

    @pl.when(step == pl.num_programs(0) - 1)
    def _():
        rows = out.shape[3]
        for core in range(2):
            for half in range(2):
                at = (2 * half + core) * rows
                out[core, half] = total[:, at : at + rows] * (1.0 / 12.0)


def lateral(orbitals, weights):
    bands, parts, planes, nx, ny = orbitals.shape
    return pl.pallas_call(
        lateral_kernel,
        grid=(bands,),
        in_specs=[
            pl.BlockSpec(memory_space=pltpu.SMEM),
            pl.BlockSpec((1, parts, planes, nx, ny), lambda n: (n, 0, 0, 0, 0)),
            pl.BlockSpec((nx, nx), lambda n: (0, 0)),
            pl.BlockSpec((ny, ny), lambda n: (0, 0)),
        ],
        out_specs=pl.BlockSpec((2, 2, 5, nx // 4, ny), lambda n: (0, 0, 0, 0, 0)),
        out_shape=jax.ShapeDtypeStruct((2, 2, 5, nx // 4, ny), jnp.float32),
        scratch_shapes=[pltpu.VMEM((5, nx, ny), jnp.float32)],
        compiler_params=pltpu.CompilerParams(vmem_limit_bytes=8 << 20),
        name="lateral",
    )(weights, orbitals, stencil(nx).T, stencil(ny))


def crossing(weight_sets, first_sets, second_sets, odd):
    rows, lanes = first_sets[0].shape[-2:]
    zero = jnp.zeros((rows, lanes), jnp.float32)
    sums = (zero, zero, zero)
    for weights, first, second in zip(weight_sets, first_sets, second_sets):

        def advance(n, sums):
            def pair(lower, upper):
                re, im = (weights[n] * first[n, part, lower].astype(jnp.float32) for part in range(2))
                re_up, im_up = (second[n, part, upper].astype(jnp.float32) for part in range(2))
                return re * im_up - im * re_up

            return (
                sums[0] + pair(0, 0),
                sums[1] + pair(1, 1),
                sums[2] + pair(1 - odd, odd),
            )

        sums = lax.fori_loop(0, first.shape[0], advance, sums, unroll=2)
    sign = (1 - 2 * odd).astype(jnp.float32) * (1.0 / 12.0)
    return sign * sums[0], sign * sums[1], (8.0 * sign) * sums[2]


def inner_kernel(flags, w1, w2, own1, own2, side1, side2, own_out, side_out):
    odd = flags[0]
    low, high, mid = crossing((w1, w2), (own1, own2), (side1, side2), odd)
    up = jnp.where(odd == 1, 1.0, 0.0)
    own_out[0] = up * mid - low
    own_out[1] = (1.0 - up) * mid - high
    side_out[0] = (1.0 - up) * mid - low
    side_out[1] = up * mid - high


def outer_kernel(flags, w1, w2, side1, side2, far1, far2, own_in, side_in, kept, near, middle, distant):
    odd = flags[0]
    corner = flags[1]
    low, high, mid = crossing((w1, w2), (side1, side2), (far1, far2), odd)
    up = jnp.where(odd == 1, 1.0, 0.0)
    own = own_in[...]
    side = side_in[...] + jnp.stack([up * mid - low, (1.0 - up) * mid - high])
    far = jnp.stack([(1.0 - up) * mid - low, up * mid - high])
    here = corner == 1
    kept[...] = jnp.where(here, own, 0.0)
    near[...] = jnp.where(here, side, own)
    middle[...] = jnp.where(here, far, side)
    distant[...] = far


def call(kernel, scalars, arrays, outs):
    smem = pl.BlockSpec(memory_space=pltpu.SMEM)
    vmem = pl.BlockSpec(memory_space=pltpu.VMEM)
    shape = arrays[0].shape
    out = jax.ShapeDtypeStruct((2,) + shape[-2:], jnp.float32)
    return pl.pallas_call(
        kernel,
        in_specs=[smem] * len(scalars) + [vmem] * len(arrays),
        out_specs=[vmem] * outs,
        out_shape=[out] * outs,
        compiler_params=pltpu.CompilerParams(vmem_limit_bytes=8 << 20),
    )(*scalars, *arrays)


def per_device(orbitals, occupations):
    slabs = lax.axis_size("grid")
    groups = lax.axis_size("band")
    assert groups == 4 and slabs % 2 == 0 and orbitals.shape[2] == 2
    slab = lax.axis_index("grid")
    group = lax.axis_index("band")
    odd = slab % 2
    core = group % 2
    half = group // 2
    corner = (half == odd).astype(jnp.int32)
    flags = jnp.stack([odd, corner]).astype(jnp.int32)
    quarter = orbitals.shape[3] // 4

    def beyond(g):
        return (g + 2) % slabs if g % 2 else (g - 2) % slabs

    def home(g):
        return (g - 2) % slabs if g % 2 else (g + 2) % slabs

    def route(value, target):
        pairs = []
        for b in range(groups):
            for g in range(slabs):
                goal = target(b, g)
                if goal is not None:
                    pairs.append((b * slabs + g, goal[0] * slabs + goal[1]))
        return lax.ppermute(value, ("band", "grid"), pairs)

    def rows(index):
        return lax.dynamic_slice_in_dim(orbitals, index * quarter, quarter, 3)

    own = rows(2 * odd + core)
    own_across = rows(2 * odd + 1 - core)
    side = rows(2 * (1 - odd) + core)
    side_across = rows(2 * (1 - odd) + 1 - core)

    side1 = route(side, lambda b, g: (b, g ^ 1))
    far1 = route(own, lambda b, g: (b, beyond(g)))
    side2 = route(side_across, lambda b, g: (b ^ 1, g ^ 1))
    far2 = route(own_across, lambda b, g: (b ^ 1, beyond(g)))
    own2 = route(own_across, lambda b, g: (b ^ 1, g))
    w2 = route(occupations, lambda b, g: (b ^ 1, g))

    flat = lateral(orbitals, occupations)
    flat = flat[core] + route(flat[1 - core], lambda b, g: (b ^ 1, g))
    flat = flat[half] + route(flat[1 - half], lambda b, g: (b ^ 2, g))

    weights = (occupations, w2)
    own_part, side_part = call(inner_kernel, (flags, *weights), (own, own2, side1, side2), 2)
    kept, near, middle, distant = call(
        outer_kernel,
        (flags, *weights),
        (side1, side2, far1, far2, own_part, side_part),
        4,
    )

    def is_corner(b, g):
        return b // 2 == g % 2

    got = route(distant, lambda b, g: None if is_corner(b, g) else (b ^ 2, home(g)))
    got_middle = route(middle, lambda b, g: (b, home(g)) if is_corner(b, g) else (b ^ 2, g ^ 1))
    got_near = route(near, lambda b, g: (b, g ^ 1) if is_corner(b, g) else (b ^ 2, g))
    depth = flat[0][None] + kept + got_near + got_middle + got
    return jnp.stack([depth, flat[1:3], flat[3:5]])


def solution(mesh):
    placed = (P("band", None, "grid", None, None), P("band"))
    return jax.shard_map(
        per_device,
        mesh=mesh,
        in_specs=placed,
        out_specs=P(None, "grid", "band", None),
        check_vma=False,
    )
```

```python
import functools

import jax
import jax.numpy as jnp
import numpy as np
from jax import lax
from jax.experimental import pallas as pl
from jax.experimental.pallas import tpu as pltpu
from jax.sharding import PartitionSpec as P


ODD, CORNER, CORE, HALF = range(4, 8)


def stencil(cells):
    eye = np.eye(cells, dtype=np.float32)
    near = np.roll(eye, 1, 0) - np.roll(eye, -1, 0)
    far = np.roll(eye, 2, 0) - np.roll(eye, -2, 0)
    return jnp.asarray(8.0 * near - far, jnp.bfloat16)


def lateral_kernel(table, weights, *rest):
    quarters, (across, along, kept, sent, spread, field, total) = rest[:4], rest[4:]
    bands, parts, planes, rows, _ = quarters[0].shape
    total[...] = jnp.zeros_like(total)
    dot = functools.partial(jnp.dot, preferred_element_type=jnp.float32)

    def advance(n, carry):
        weight = weights[n]
        for i, quarter in enumerate(quarters):
            at = pl.ds(pl.multiple_of(table[i] * rows, rows), rows)
            for part in range(parts):
                for plane in range(planes):
                    field[part, plane, at] = quarter[n, part, plane]
        fields = []
        for plane in range(planes):
            re16 = field[0, plane]
            im16 = field[1, plane]
            re = weight * re16.astype(jnp.float32)
            im = weight * im16.astype(jnp.float32)
            fields.append((re, im, re16, im16))
            total[1 + plane] += re * dot(across[...], im16) - im * dot(across[...], re16)
            total[3 + plane] += re * dot(im16, along[...]) - im * dot(re16, along[...])
        (re, im, _, _), (_, _, re_up, im_up) = fields
        total[0] += 8.0 * (re * im_up.astype(jnp.float32) - im * re_up.astype(jnp.float32))
        return carry

    lax.fori_loop(0, bands, advance, 0)
    for n in range(bands):
        spread[n : n + 1] = jnp.full((1, spread.shape[1]), weights[n], jnp.float32)
    core = table[CORE]
    for half in range(2):
        for out, row in ((kept, 2 * half + core), (sent, 2 * half + 1 - core)):
            at = pl.ds(pl.multiple_of(row * rows, rows), rows)
            out[half] = total[:, at] * (1.0 / 12.0)


def lateral(quarters, table, weights):
    bands, parts, planes, rows, ny = quarters[0].shape
    nx = 4 * rows
    smem = pl.BlockSpec(memory_space=pltpu.SMEM)
    vmem = pl.BlockSpec(memory_space=pltpu.VMEM)
    return pl.pallas_call(
        lateral_kernel,
        in_specs=[smem] * 2 + [vmem] * 6,
        out_specs=[vmem] * 3,
        out_shape=[jax.ShapeDtypeStruct((2, 5, rows, ny), jnp.float32)] * 2
        + [jax.ShapeDtypeStruct((bands, ny), jnp.float32)],
        scratch_shapes=[
            pltpu.VMEM((parts, planes, nx, ny), quarters[0].dtype),
            pltpu.VMEM((5, nx, ny), jnp.float32),
        ],
        compiler_params=pltpu.CompilerParams(vmem_limit_bytes=8 << 20),
        name="lateral",
    )(table, weights, *quarters, stencil(nx).T, stencil(ny))


def split_kernel(table, orbitals, *rest):
    outs, flags, sem = rest[:4], rest[4], rest[5]
    rows = outs[0].shape[3]
    copies = [
        pltpu.make_async_copy(
            orbitals.at[:, :, :, pl.ds(pl.multiple_of(table[i] * rows, rows), rows)], out, sem.at[i]
        )
        for i, out in enumerate(outs)
    ]
    for copy in copies:
        copy.start()
    for i in range(flags.shape[0]):
        flags[i : i + 1] = jnp.full((1, flags.shape[1]), table[i], jnp.int32)
    for copy in copies:
        copy.wait()


def split(table, orbitals):
    bands, parts, planes, nx, ny = orbitals.shape
    smem = pl.BlockSpec(memory_space=pltpu.SMEM)
    vmem = pl.BlockSpec(memory_space=pltpu.VMEM)
    return pl.pallas_call(
        split_kernel,
        in_specs=[smem, pl.BlockSpec(memory_space=pltpu.HBM)],
        out_specs=[vmem] * 5,
        out_shape=[pltpu.VMEM((bands, parts, planes, nx // 4, ny), orbitals.dtype)] * 4
        + [pltpu.VMEM((8, ny), jnp.int32)],
        scratch_shapes=[pltpu.SemaphoreType.DMA((4,))],
        compiler_params=pltpu.CompilerParams(vmem_limit_bytes=4 << 20),
        name="split",
    )(table, pltpu.with_memory_space_constraint(orbitals, pltpu.HBM))


def halve_kernel(flags, mine, theirs, kept, sent):
    lower = jnp.broadcast_to(flags[HALF : HALF + 1], kept.shape[1:]) == 0
    for i in range(kept.shape[0]):
        low = mine[0, i] + theirs[0, i]
        high = mine[1, i] + theirs[1, i]
        kept[i] = jnp.where(lower, low, high)
        sent[i] = jnp.where(lower, high, low)


def edges(odd, weights, own, side, far, sums):
    def advance(n, sums):
        def field(rows):
            planes = [[rows[n, part, k].astype(jnp.float32) for part in range(2)] for k in range(2)]
            return planes

        def pick(low, high):
            return [jnp.where(odd, a, b) for a, b in zip(low, high)]

        def term(first, second):
            return weight * (first[0] * second[1] - first[1] * second[0])

        weight = weights[pl.ds(n, 1)]
        o, s, f = field(own), field(side), field(far)
        lower = pick(s[0], s[1])
        upper = pick(s[1], s[0])
        new = (
            term(o[0], s[0]),
            term(o[1], s[1]),
            term(pick(o[0], o[1]), upper),
            term(s[0], f[0]),
            term(s[1], f[1]),
            term(lower, pick(f[1], f[0])),
        )
        return tuple(a + b for a, b in zip(sums, new))

    return lax.fori_loop(0, own.shape[0], advance, sums, unroll=UNROLL)


def first_kernel(flags, weights, own, side, far, out):
    zero = jnp.zeros(out.shape[1:], jnp.float32)
    odd = jnp.broadcast_to(flags[ODD : ODD + 1], out.shape[1:]) == 1
    for i, value in enumerate(edges(odd, weights, own, side, far, (zero,) * 6)):
        out[i] = value


def second_kernel(flags, weights, own, side, far, sums, kept, near, middle, distant):
    shape = kept.shape[1:]
    odd = jnp.broadcast_to(flags[ODD : ODD + 1], shape) == 1
    here = jnp.broadcast_to(flags[CORNER : CORNER + 1], shape) == 1
    sums = edges(odd, weights, own, side, far, tuple(sums[i] for i in range(6)))
    up = jnp.where(odd, 1.0, 0.0)
    down = 1.0 - up
    sign = (down - up) * (1.0 / 12.0)
    low, high, mid, far_low, far_high, far_mid = (
        value * (sign if i % 3 < 2 else 8.0 * sign) for i, value in enumerate(sums)
    )
    own_parts = (up * mid - low, down * mid - high)
    side_parts = (
        down * mid - low + up * far_mid - far_low,
        up * mid - high + down * far_mid - far_high,
    )
    far_parts = (down * far_mid - far_low, up * far_mid - far_high)
    for plane in range(2):
        kept[plane] = jnp.where(here, own_parts[plane], 0.0)
        near[plane] = jnp.where(here, side_parts[plane], own_parts[plane])
        middle[plane] = jnp.where(here, far_parts[plane], side_parts[plane])
        distant[plane] = far_parts[plane]


def call(kernel, arrays, out_shapes):
    vmem = pl.BlockSpec(memory_space=pltpu.VMEM)
    return pl.pallas_call(
        kernel,
        in_specs=[vmem] * len(arrays),
        out_specs=[vmem] * len(out_shapes),
        out_shape=[jax.ShapeDtypeStruct(shape, jnp.float32) for shape in out_shapes],
        compiler_params=pltpu.CompilerParams(vmem_limit_bytes=4 << 20),
    )(*arrays)


def finish_kernel(flags, flat, flat_rest, kept, near, middle, distant, out):
    here = jnp.broadcast_to(flags[CORNER : CORNER + 1], flat.shape[1:]) == 1
    for plane in range(2):
        total = flat[0] + flat_rest[0] + kept[plane] + near[plane] + middle[plane]
        out[0, plane] = total + jnp.where(here, distant[plane], 0.0)
        out[1, plane] = flat[1 + plane] + flat_rest[1 + plane]
        out[2, plane] = flat[3 + plane] + flat_rest[3 + plane]


def per_device(orbitals, occupations):
    slabs = lax.axis_size("grid")
    groups = lax.axis_size("band")
    assert groups == 4 and slabs % 2 == 0 and orbitals.shape[2] == 2
    slab = lax.axis_index("grid")
    group = lax.axis_index("band")
    odd = slab % 2
    core = group % 2
    half = group // 2
    corner = (half == odd).astype(odd.dtype)

    def beyond(g):
        return (g + 2) % slabs if g % 2 else (g - 2) % slabs

    def home(g):
        return (g - 2) % slabs if g % 2 else (g + 2) % slabs

    def route(value, target):
        pairs = []
        for b in range(groups):
            for g in range(slabs):
                goal = target(b, g)
                pairs.append((b * slabs + g, goal[0] * slabs + goal[1]))
        return lax.ppermute(value, ("band", "grid"), pairs)

    table = jnp.stack(
        [
            2 * odd + core,
            2 * (1 - odd) + core,
            2 * odd + 1 - core,
            2 * (1 - odd) + 1 - core,
            odd,
            corner,
            core,
            half,
        ]
    ).astype(jnp.int32)
    own, side, own_across, side_across, flags = split(table, orbitals)

    side1 = route(side, lambda b, g: (b, g ^ 1))
    far1 = route(own, lambda b, g: (b, beyond(g)))
    side2 = route(side_across, lambda b, g: (b ^ 1, g ^ 1))
    far2 = route(own_across, lambda b, g: (b ^ 1, beyond(g)))
    own2 = route(own_across, lambda b, g: (b ^ 1, g))

    plane = own.shape[-2:]
    mine, sent, spread = lateral((own, side, own_across, side_across), table, occupations)
    w2 = route(spread, lambda b, g: (b ^ 1, g))
    theirs = route(sent, lambda b, g: (b ^ 1, g))
    flat, sent = call(halve_kernel, (flags, mine, theirs), [(5,) + plane] * 2)
    flat_rest = route(sent, lambda b, g: (b ^ 2, g))

    (sums,) = call(first_kernel, (flags, spread, own, side1, far1), [(6,) + plane])
    kept, near, middle, distant = call(
        second_kernel, (flags, w2, own2, side2, far2, sums), [(2,) + plane] * 4
    )

    def is_corner(b, g):
        return b // 2 == g % 2

    got_near = route(near, lambda b, g: (b, g ^ 1) if is_corner(b, g) else (b ^ 2, g))
    got_middle = route(middle, lambda b, g: (b, home(g)) if is_corner(b, g) else (b ^ 2, g ^ 1))
    got = route(distant, lambda b, g: (b ^ 2, home(g)))
    (out,) = call(finish_kernel, (flags, flat, flat_rest, kept, got_near, got_middle, got), [(3, 2) + plane])
    return out


UNROLL = 4


def solution(mesh):
    placed = (P("band", None, "grid", None, None), P("band"))
    return jax.shard_map(
        per_device,
        mesh=mesh,
        in_specs=placed,
        out_specs=P(None, "grid", "band", None),
        check_vma=False,
    )
```

```python
import functools

import jax
import jax.numpy as jnp
import numpy as np
from jax import lax
from jax.experimental import pallas as pl
from jax.experimental.pallas import tpu as pltpu
from jax.sharding import PartitionSpec as P


ODD, CORNER, CORE, HALF = range(4, 8)


def stencil(cells):
    eye = np.eye(cells, dtype=np.float32)
    near = np.roll(eye, 1, 0) - np.roll(eye, -1, 0)
    far = np.roll(eye, 2, 0) - np.roll(eye, -2, 0)
    return jnp.asarray(8.0 * near - far, jnp.bfloat16)


def lateral_kernel(weights, *rest):
    quarters, (across, along, kept, sent, spread, field, total) = rest[:4], rest[4:]
    bands, parts, planes, rows, _ = quarters[0].shape
    table = places()
    total[...] = jnp.zeros_like(total)
    dot = functools.partial(jnp.dot, preferred_element_type=jnp.float32)

    def advance(n, carry):
        weight = weights[n]
        for i, quarter in enumerate(quarters):
            at = pl.ds(pl.multiple_of(table[i] * rows, rows), rows)
            for part in range(parts):
                for plane in range(planes):
                    field[part, plane, at] = quarter[n, part, plane]
        fields = []
        for plane in range(planes):
            re16 = field[0, plane]
            im16 = field[1, plane]
            re = weight * re16.astype(jnp.float32)
            im = weight * im16.astype(jnp.float32)
            fields.append((re, im, re16, im16))
            total[1 + plane] += re * dot(across[...], im16) - im * dot(across[...], re16)
            total[3 + plane] += re * dot(im16, along[...]) - im * dot(re16, along[...])
        (re, im, _, _), (_, _, re_up, im_up) = fields
        total[0] += 8.0 * (re * im_up.astype(jnp.float32) - im * re_up.astype(jnp.float32))
        return carry

    lax.fori_loop(0, bands, advance, 0)
    for n in range(bands):
        spread[n : n + 1] = jnp.full((1, spread.shape[1]), weights[n], jnp.float32)
    core = table[CORE]
    for half in range(2):
        for out, row in ((kept, 2 * half + core), (sent, 2 * half + 1 - core)):
            at = pl.ds(pl.multiple_of(row * rows, rows), rows)
            out[half] = total[:, at] * (1.0 / 12.0)


def lateral(quarters, weights):
    bands, parts, planes, rows, ny = quarters[0].shape
    nx = 4 * rows
    smem = pl.BlockSpec(memory_space=pltpu.SMEM)
    vmem = pl.BlockSpec(memory_space=pltpu.VMEM)
    return pl.pallas_call(
        lateral_kernel,
        in_specs=[smem] + [vmem] * 6,
        out_specs=[vmem] * 3,
        out_shape=[jax.ShapeDtypeStruct((2, 5, rows, ny), jnp.float32)] * 2
        + [jax.ShapeDtypeStruct((bands, ny), jnp.float32)],
        scratch_shapes=[
            pltpu.VMEM((parts, planes, nx, ny), quarters[0].dtype),
            pltpu.VMEM((5, nx, ny), jnp.float32),
        ],
        compiler_params=pltpu.CompilerParams(vmem_limit_bytes=8 << 20),
        name="lateral",
    )(weights, *quarters, stencil(nx).T, stencil(ny))


def places():
    odd = lax.axis_index("grid") % 2
    group = lax.axis_index("band")
    core = group % 2
    half = group // 2
    quarters = (
        2 * (1 - odd) + core,
        2 * odd + core,
        2 * (1 - odd) + 1 - core,
        2 * odd + 1 - core,
    )
    corner = jnp.where(half == odd, 0, 1)
    return quarters + (odd, corner, core, half)


def split_kernel(first, orbitals, *rest):
    outs, flags, sem = rest[:2], rest[2], rest[3]
    rows = outs[0].shape[3]
    table = places()
    copies = [
        pltpu.make_async_copy(
            orbitals.at[:, :, :, pl.ds(pl.multiple_of(table[first + i] * rows, rows), rows)], out, sem.at[i]
        )
        for i, out in enumerate(outs)
    ]
    for copy in copies:
        copy.start()
    for i, place in enumerate(table):
        flags[i : i + 1] = jnp.full((1, flags.shape[1]), place, jnp.int32)
    for copy in copies:
        copy.wait()


def split(first, orbitals):
    bands, parts, planes, nx, ny = orbitals.shape
    return pl.pallas_call(
        functools.partial(split_kernel, first),
        in_specs=[pl.BlockSpec(memory_space=pltpu.HBM)],
        out_specs=[pl.BlockSpec(memory_space=pltpu.VMEM)] * 3,
        out_shape=[pltpu.VMEM((bands, parts, planes, nx // 4, ny), orbitals.dtype)] * 2
        + [pltpu.VMEM((8, ny), jnp.int32)],
        scratch_shapes=[pltpu.SemaphoreType.DMA((2,))],
        compiler_params=pltpu.CompilerParams(vmem_limit_bytes=4 << 20),
        name="split",
    )(pltpu.with_memory_space_constraint(orbitals, pltpu.HBM))


def halve_kernel(flags, mine, theirs, kept, sent):
    lower = jnp.broadcast_to(flags[HALF : HALF + 1], kept.shape[1:]) == 0
    for i in range(kept.shape[0]):
        low = mine[0, i] + theirs[0, i]
        high = mine[1, i] + theirs[1, i]
        kept[i] = jnp.where(lower, low, high)
        sent[i] = jnp.where(lower, high, low)


def edges(odd, weights, first, second, sums):
    def advance(n, sums):
        def field(rows, scale=None):
            values = [[rows[n, part, k].astype(jnp.float32) for part in range(2)] for k in range(2)]
            if scale is not None:
                values = [[scale * value for value in plane] for plane in values]
            return values

        def pick(low, high):
            return [jnp.where(odd, a, b) for a, b in zip(low, high)]

        def term(low, high):
            return low[0] * high[1] - low[1] * high[0]

        f, g = field(first, weights[pl.ds(n, 1)]), field(second)
        new = (
            term(f[0], g[0]),
            term(f[1], g[1]),
            term(pick(f[0], f[1]), pick(g[1], g[0])),
        )
        return tuple(a + b for a, b in zip(sums, new))

    sums = tuple(sums[i] for i in range(3))
    return lax.fori_loop(0, first.shape[0], advance, sums, unroll=UNROLL)


def flag(flags, which, shape):
    return jnp.broadcast_to(flags[which : which + 1], shape) == 1


def scaled(odd, sums):
    sign = jnp.where(odd, -1.0 / 12.0, 1.0 / 12.0)
    low, high, mid = sums
    up = jnp.where(odd, -8.0 / 12.0, 0.0) * mid
    down = jnp.where(odd, 0.0, 8.0 / 12.0) * mid
    return (up - sign * low, down - sign * high), (down - sign * low, up - sign * high)


def first_kernel(flags, weights, own, side, far, inner, outer):
    shape = inner.shape[1:]
    odd = flag(flags, ODD, shape)
    zero = (jnp.zeros(shape, jnp.float32),) * 3
    for out, pair in ((inner, (own, side)), (outer, (side, far))):
        for i, value in enumerate(edges(odd, weights, *pair, zero)):
            out[i] = value


def inner_kernel(flags, weights, own, side, sums, kept, near, inner_side):
    shape = kept.shape[1:]
    odd = flag(flags, ODD, shape)
    here = flag(flags, CORNER, shape)
    own_parts, side_parts = scaled(odd, edges(odd, weights, own, side, sums))
    for plane in range(2):
        kept[plane] = jnp.where(here, own_parts[plane], 0.0)
        near[plane] = jnp.where(here, side_parts[plane], own_parts[plane])
        inner_side[plane] = side_parts[plane]


def outer_kernel(flags, weights, side, far, sums, inner_side, middle, distant):
    shape = middle.shape[1:]
    odd = flag(flags, ODD, shape)
    here = flag(flags, CORNER, shape)
    side_parts, far_parts = scaled(odd, edges(odd, weights, side, far, sums))
    for plane in range(2):
        middle[plane] = jnp.where(here, far_parts[plane], side_parts[plane] + inner_side[plane])
        distant[plane] = jnp.where(here, side_parts[plane], far_parts[plane])


def call(kernel, arrays, out_shapes):
    vmem = pl.BlockSpec(memory_space=pltpu.VMEM)
    return pl.pallas_call(
        kernel,
        in_specs=[vmem] * len(arrays),
        out_specs=[vmem] * len(out_shapes),
        out_shape=[jax.ShapeDtypeStruct(shape, jnp.float32) for shape in out_shapes],
        compiler_params=pltpu.CompilerParams(vmem_limit_bytes=4 << 20),
    )(*arrays)


def finish_kernel(flat, flat_rest, kept, near, middle, distant, out):
    for plane in range(2):
        parts = kept[plane] + near[plane] + middle[plane] + distant[plane]
        out[0, plane] = flat[0] + flat_rest[0] + parts
        out[1, plane] = flat[1 + plane] + flat_rest[1 + plane]
        out[2, plane] = flat[3 + plane] + flat_rest[3 + plane]


def per_device(orbitals, occupations):
    slabs = lax.axis_size("grid")
    groups = lax.axis_size("band")
    assert groups == 4 and slabs % 2 == 0 and orbitals.shape[2] == 2

    def beyond(g):
        return (g + 2) % slabs if g % 2 else (g - 2) % slabs

    def home(g):
        return (g - 2) % slabs if g % 2 else (g + 2) % slabs

    def route(value, target):
        pairs = []
        for b in range(groups):
            for g in range(slabs):
                goal = target(b, g)
                pairs.append((b * slabs + g, goal[0] * slabs + goal[1]))
        return lax.ppermute(value, ("band", "grid"), pairs)

    own, side, flags = split(0, orbitals)
    own_across, side_across, _ = split(2, orbitals)

    side1 = route(side, lambda b, g: (b, g ^ 1))
    far1 = route(own, lambda b, g: (b, beyond(g)))
    side2 = route(side_across, lambda b, g: (b ^ 1, g ^ 1))
    far2 = route(own_across, lambda b, g: (b ^ 1, beyond(g)))
    own2 = route(own_across, lambda b, g: (b ^ 1, g))

    plane = own.shape[-2:]
    mine, sent, spread = lateral((own, side, own_across, side_across), occupations)
    w2 = route(spread, lambda b, g: (b ^ 1, g))
    theirs = route(sent, lambda b, g: (b ^ 1, g))
    flat, sent = call(halve_kernel, (flags, mine, theirs), [(5,) + plane] * 2)
    flat_rest = route(sent, lambda b, g: (b ^ 2, g))

    inner, outer = call(
        first_kernel, (flags, spread, own, side1, far1), [(3,) + plane] * 2
    )
    kept, near, inner_side = call(inner_kernel, (flags, w2, own2, side2, inner), [(2,) + plane] * 3)

    def is_corner(b, g):
        return b // 2 != g % 2

    got_near = route(near, lambda b, g: (b, g ^ 1) if is_corner(b, g) else (b ^ 2, g))
    middle, distant = call(
        outer_kernel, (flags, w2, side2, far2, outer, inner_side), [(2,) + plane] * 2
    )
    got_middle = route(middle, lambda b, g: (b, home(g)) if is_corner(b, g) else (b ^ 2, g ^ 1))
    got_distant = route(distant, lambda b, g: (b, g ^ 1) if is_corner(b, g) else (b ^ 2, home(g)))
    arrays = (flat, flat_rest, kept, got_near, got_middle, got_distant)
    (out,) = call(finish_kernel, arrays, [(3, 2) + plane])
    return out


UNROLL = 4


def solution(mesh):
    placed = (P("band", None, "grid", None, None), P("band"))
    return jax.shard_map(
        per_device,
        mesh=mesh,
        in_specs=placed,
        out_specs=P(None, "grid", "band", None),
        check_vma=False,
    )
```

```python
import functools

import jax
import jax.numpy as jnp
import numpy as np
from jax import lax
from jax.experimental import pallas as pl
from jax.experimental.pallas import tpu as pltpu
from jax.sharding import PartitionSpec as P


ODD, CORNER, CORE, HALF, SWAP = range(4, 9)


def stencil(cells):
    eye = np.eye(cells, dtype=np.float32)
    near = np.roll(eye, 1, 0) - np.roll(eye, -1, 0)
    far = np.roll(eye, 2, 0) - np.roll(eye, -2, 0)
    return jnp.asarray(8.0 * near - far, jnp.bfloat16)


def lateral_kernel(weights, *rest):
    quarters, (across, along, kept, sent, spread, field, total) = rest[:4], rest[4:]
    bands, parts, planes, rows, _ = quarters[0].shape
    table = places()
    total[...] = jnp.zeros_like(total)
    dot = functools.partial(jnp.dot, preferred_element_type=jnp.float32)

    def advance(n, carry):
        weight = weights[n]
        for i, quarter in enumerate(quarters):
            at = pl.ds(pl.multiple_of(table[i] * rows, rows), rows)
            for part in range(parts):
                for plane in range(planes):
                    field[part, plane, at] = quarter[n, part, plane]
        fields = []
        for plane in range(planes):
            re16 = field[0, plane]
            im16 = field[1, plane]
            re = weight * re16.astype(jnp.float32)
            im = weight * im16.astype(jnp.float32)
            fields.append((re, im, re16, im16))
            total[1 + plane] += re * dot(across[...], im16) - im * dot(across[...], re16)
            total[3 + plane] += re * dot(im16, along[...]) - im * dot(re16, along[...])
        (re, im, _, _), (_, _, re_up, im_up) = fields
        total[0] += 8.0 * (re * im_up.astype(jnp.float32) - im * re_up.astype(jnp.float32))
        return carry

    lax.fori_loop(0, bands, advance, 0)
    for n in range(bands):
        spread[n : n + 1] = jnp.full((1, spread.shape[1]), weights[n], jnp.float32)
    core = table[CORE]
    for half in range(2):
        for out, row in ((kept, 2 * half + core), (sent, 2 * half + 1 - core)):
            at = pl.ds(pl.multiple_of(row * rows, rows), rows)
            out[half] = total[:, at] * (1.0 / 12.0)


def lateral(quarters, weights):
    bands, parts, planes, rows, ny = quarters[0].shape
    nx = 4 * rows
    smem = pl.BlockSpec(memory_space=pltpu.SMEM)
    vmem = pl.BlockSpec(memory_space=pltpu.VMEM)
    return pl.pallas_call(
        lateral_kernel,
        in_specs=[smem] + [vmem] * 6,
        out_specs=[vmem] * 3,
        out_shape=[jax.ShapeDtypeStruct((2, 5, rows, ny), jnp.float32)] * 2
        + [jax.ShapeDtypeStruct((bands, ny), jnp.float32)],
        scratch_shapes=[
            pltpu.VMEM((parts, planes, nx, ny), quarters[0].dtype),
            pltpu.VMEM((5, nx, ny), jnp.float32),
        ],
        compiler_params=pltpu.CompilerParams(vmem_limit_bytes=8 << 20),
        name="lateral",
    )(weights, *quarters, stencil(nx).T, stencil(ny))


def ends():
    slab = lax.axis_index("grid")
    levels = lax.axis_size("grid") // 2
    odd = slab % 2
    below = slab // 2
    above = lax.rem(below + 1, levels)
    leave = jnp.where(odd == 1, above, below)
    enter = jnp.where(odd == 1, below, above)
    return any_of(leave, FIRST, levels), any_of(enter, FIRST, levels)


def any_of(cycle, members, levels):
    found = cycle < 0
    for member in members:
        found = found | (cycle == member % levels)
    return found


def places():
    odd = lax.axis_index("grid") % 2
    group = lax.axis_index("band")
    core = group % 2
    half = group // 2
    own = 2 * (1 - odd) + core
    side = 2 * odd + core
    sends, _ = ends()
    quarters = (
        jnp.where(sends, own, side),
        jnp.where(sends, side, own),
        2 * (1 - odd) + 1 - core,
        2 * odd + 1 - core,
    )
    corner = jnp.where(half == odd, 0, 1)
    ahead = corner
    for slab in CELLS:
        at = lax.axis_index("grid") == slab % lax.axis_size("grid")
        ahead = jnp.where(at, 1 - ahead, ahead)
    return quarters + (odd, corner, core, half, ahead)


def split_kernel(first, orbitals, *rest):
    outs, flags, sem = rest[:2], rest[2], rest[3]
    rows = outs[0].shape[3]
    table = places()
    copies = [
        pltpu.make_async_copy(
            orbitals.at[:, :, :, pl.ds(pl.multiple_of(table[first + i] * rows, rows), rows)], out, sem.at[i]
        )
        for i, out in enumerate(outs)
    ]
    for copy in copies:
        copy.start()
    for i, place in enumerate(table):
        flags[i : i + 1] = jnp.full((1, flags.shape[1]), place, jnp.int32)
    for copy in copies:
        copy.wait()


def split(first, orbitals):
    bands, parts, planes, nx, ny = orbitals.shape
    return pl.pallas_call(
        functools.partial(split_kernel, first),
        in_specs=[pl.BlockSpec(memory_space=pltpu.HBM)],
        out_specs=[pl.BlockSpec(memory_space=pltpu.VMEM)] * 3,
        out_shape=[pltpu.VMEM((bands, parts, planes, nx // 4, ny), orbitals.dtype)] * 2
        + [pltpu.VMEM((16, ny), jnp.int32)],
        scratch_shapes=[pltpu.SemaphoreType.DMA((2,))],
        compiler_params=pltpu.CompilerParams(vmem_limit_bytes=4 << 20),
        name="split",
    )(pltpu.with_memory_space_constraint(orbitals, pltpu.HBM))


def halve_kernel(flags, mine, theirs, kept, sent):
    lower = jnp.broadcast_to(flags[HALF : HALF + 1], kept.shape[1:]) == 0
    for i in range(kept.shape[0]):
        low = mine[0, i] + theirs[0, i]
        high = mine[1, i] + theirs[1, i]
        kept[i] = jnp.where(lower, low, high)
        sent[i] = jnp.where(lower, high, low)


def edges(odd, weights, first, second, sums):
    def advance(n, sums):
        def field(rows, scale=None):
            values = [[rows[n, part, k].astype(jnp.float32) for part in range(2)] for k in range(2)]
            if scale is not None:
                values = [[scale * value for value in plane] for plane in values]
            return values

        def pick(low, high):
            return [jnp.where(odd, a, b) for a, b in zip(low, high)]

        def term(low, high):
            return low[0] * high[1] - low[1] * high[0]

        f, g = field(first, weights[pl.ds(n, 1)]), field(second)
        new = (
            term(f[0], g[0]),
            term(f[1], g[1]),
            term(pick(f[0], f[1]), pick(g[1], g[0])),
        )
        return tuple(a + b for a, b in zip(sums, new))

    sums = tuple(sums[i] for i in range(3))
    return lax.fori_loop(0, first.shape[0], advance, sums, unroll=UNROLL)


def flag(flags, which, shape):
    return jnp.broadcast_to(flags[which : which + 1], shape) == 1


def scaled(odd, sums):
    sign = jnp.where(odd, -1.0 / 12.0, 1.0 / 12.0)
    low, high, mid = sums
    up = jnp.where(odd, -8.0 / 12.0, 0.0) * mid
    down = jnp.where(odd, 0.0, 8.0 / 12.0) * mid
    return (up - sign * low, down - sign * high), (down - sign * low, up - sign * high)


def first_kernel(flags, weights, lead, trail, got_lead, got_trail, inner, outer):
    shape = inner.shape[1:]
    odd = flag(flags, ODD, shape)
    zero = (jnp.zeros(shape, jnp.float32),) * 3
    sends, receives = ends()

    def run(own, side, far):
        for out, pair in ((inner, (own, side)), (outer, (side, far))):
            for i, value in enumerate(edges(odd, weights, *pair, zero)):
                out[i] = value

    for one in (sends, jnp.logical_not(sends)):
        for two in (receives, jnp.logical_not(receives)):
            own = lead if one is sends else trail
            side, far = (got_trail, got_lead) if two is receives else (got_lead, got_trail)
            pl.when(one & two)(functools.partial(run, own, side, far))


def inner_kernel(flags, weights, own, side, sums, kept, near, inner_side):
    shape = kept.shape[1:]
    odd = flag(flags, ODD, shape)
    here = flag(flags, CORNER, shape)
    own_parts, side_parts = scaled(odd, edges(odd, weights, own, side, sums))
    for plane in range(2):
        kept[plane] = jnp.where(here, own_parts[plane], 0.0)
        near[plane] = jnp.where(here, side_parts[plane], own_parts[plane])
        inner_side[plane] = side_parts[plane]


def outer_kernel(flags, weights, side, far, sums, inner_side, middle, distant):
    shape = middle.shape[1:]
    odd = flag(flags, ODD, shape)
    here = flag(flags, CORNER, shape)
    side_parts, far_parts = scaled(odd, edges(odd, weights, side, far, sums))
    ahead = flag(flags, SWAP, shape)
    for plane in range(2):
        beside = side_parts[plane] + jnp.where(here, 0.0, inner_side[plane])
        middle[plane] = jnp.where(ahead, beside, far_parts[plane])
        distant[plane] = jnp.where(ahead, far_parts[plane], beside)


def call(kernel, arrays, out_shapes):
    vmem = pl.BlockSpec(memory_space=pltpu.VMEM)
    return pl.pallas_call(
        kernel,
        in_specs=[vmem] * len(arrays),
        out_specs=[vmem] * len(out_shapes),
        out_shape=[jax.ShapeDtypeStruct(shape, jnp.float32) for shape in out_shapes],
        compiler_params=pltpu.CompilerParams(vmem_limit_bytes=4 << 20),
    )(*arrays)


def finish_kernel(flat, flat_rest, kept, near, middle, distant, out):
    for plane in range(2):
        parts = kept[plane] + near[plane] + middle[plane] + distant[plane]
        out[0, plane] = flat[0] + flat_rest[0] + parts
        out[1, plane] = flat[1 + plane] + flat_rest[1 + plane]
        out[2, plane] = flat[3 + plane] + flat_rest[3 + plane]


def per_device(orbitals, occupations):
    slabs = lax.axis_size("grid")
    groups = lax.axis_size("band")
    assert groups == 4 and slabs % 2 == 0 and slabs >= 4 and orbitals.shape[2] == 2

    def beyond(g):
        return (g + 2) % slabs if g % 2 else (g - 2) % slabs

    def home(g):
        return (g - 2) % slabs if g % 2 else (g + 2) % slabs

    def route(value, target):
        pairs = []
        for b in range(groups):
            for g in range(slabs):
                goal = target(b, g)
                pairs.append((b * slabs + g, goal[0] * slabs + goal[1]))
        return lax.ppermute(value, ("band", "grid"), pairs)

    lead, trail, flags = split(0, orbitals)
    own_across, side_across, _ = split(2, orbitals)

    def at_end(g):
        levels = slabs // 2
        return (g // 2 + g % 2) % levels in [member % levels for member in FIRST]

    got_lead = route(lead, lambda b, g: (b, beyond(g) if at_end(g) else g ^ 1))
    got_trail = route(trail, lambda b, g: (b, g ^ 1 if at_end(g) else beyond(g)))
    side2 = route(side_across, lambda b, g: (b ^ 1, g ^ 1))
    far2 = route(own_across, lambda b, g: (b ^ 1, beyond(g)))
    own2 = route(own_across, lambda b, g: (b ^ 1, g))

    plane = lead.shape[-2:]
    mine, sent, spread = lateral((lead, trail, own_across, side_across), occupations)
    w2 = route(spread, lambda b, g: (b ^ 1, g))
    theirs = route(sent, lambda b, g: (b ^ 1, g))
    flat, sent = call(halve_kernel, (flags, mine, theirs), [(5,) + plane] * 2)
    flat_rest = route(sent, lambda b, g: (b ^ 2, g))

    inner, outer = call(
        first_kernel, (flags, spread, lead, trail, got_lead, got_trail), [(3,) + plane] * 2
    )
    kept, near, inner_side = call(inner_kernel, (flags, w2, own2, side2, inner), [(2,) + plane] * 3)

    def is_corner(b, g):
        return b // 2 != g % 2

    got_near = route(near, lambda b, g: (b, g ^ 1) if is_corner(b, g) else (b ^ 2, g))
    middle, distant = call(
        outer_kernel, (flags, w2, side2, far2, outer, inner_side), [(2,) + plane] * 2
    )

    def beside(b, g):
        return (b, g ^ 1) if is_corner(b, g) else (b ^ 2, g ^ 1)

    def upward(b, g):
        return (b, home(g)) if is_corner(b, g) else (b ^ 2, home(g))

    def ahead(b, g):
        return is_corner(b, g) != (g in [slab % slabs for slab in CELLS])

    got_middle = route(middle, lambda b, g: beside(b, g) if ahead(b, g) else upward(b, g))
    got_distant = route(distant, lambda b, g: upward(b, g) if ahead(b, g) else beside(b, g))
    arrays = (flat, flat_rest, kept, got_near, got_middle, got_distant)
    (out,) = call(finish_kernel, arrays, [(3, 2) + plane])
    return out


FIRST = (-1,)
CELLS = (1, -1)
UNROLL = 4
FIRST = (-1,)
CELLS = (1, -1)


def solution(mesh):
    placed = (P("band", None, "grid", None, None), P("band"))
    return jax.shard_map(
        per_device,
        mesh=mesh,
        in_specs=placed,
        out_specs=P(None, "grid", "band", None),
        check_vma=False,
    )
```

```python
import functools

import jax
import jax.numpy as jnp
import numpy as np
from jax import lax
from jax.experimental import pallas as pl
from jax.experimental.pallas import tpu as pltpu
from jax.sharding import PartitionSpec as P


ODD, CORNER, CORE, HALF, SWAP, OWN, SIDE = range(4, 11)


def stencil(cells):
    eye = np.eye(cells, dtype=np.float32)
    near = np.roll(eye, 1, 0) - np.roll(eye, -1, 0)
    far = np.roll(eye, 2, 0) - np.roll(eye, -2, 0)
    return jnp.asarray(8.0 * near - far, jnp.bfloat16)


def lateral_kernel(pieces, weights, *rest):
    count = len(pieces)
    arrays, (across, along, kept, sent, spread, field, total) = rest[:count], rest[count:]
    _, parts, planes, rows, _ = arrays[0].shape
    bands = max(stop for _, _, stop in pieces)
    table = places()
    total[...] = jnp.zeros_like(total)
    dot = functools.partial(jnp.dot, preferred_element_type=jnp.float32)

    def advance(start, stop, n, carry):
        weight = weights[n]
        for array, (quarter, low, high) in zip(arrays, pieces):
            if low <= start and stop <= high:
                at = pl.ds(pl.multiple_of(table[quarter] * rows, rows), rows)
                for part in range(parts):
                    for plane in range(planes):
                        field[part, plane, at] = array[n - low, part, plane]
        fields = []
        for plane in range(planes):
            re16 = field[0, plane]
            im16 = field[1, plane]
            re = weight * re16.astype(jnp.float32)
            im = weight * im16.astype(jnp.float32)
            fields.append((re, im, re16, im16))
            total[1 + plane] += re * dot(across[...], im16) - im * dot(across[...], re16)
            total[3 + plane] += re * dot(im16, along[...]) - im * dot(re16, along[...])
        (re, im, _, _), (_, _, re_up, im_up) = fields
        total[0] += 8.0 * (re * im_up.astype(jnp.float32) - im * re_up.astype(jnp.float32))
        return carry

    cuts = sorted({cut for _, low, high in pieces for cut in (low, high)})
    for start, stop in zip(cuts, cuts[1:]):
        lax.fori_loop(start, stop, functools.partial(advance, start, stop), 0)
    for n in range(bands):
        spread[n : n + 1] = jnp.full((1, spread.shape[1]), weights[n], jnp.float32)
    core = table[CORE]
    for half in range(2):
        for out, row in ((kept, 2 * half + core), (sent, 2 * half + 1 - core)):
            at = pl.ds(pl.multiple_of(row * rows, rows), rows)
            out[half] = total[:, at] * (1.0 / 12.0)


def lateral(pieces, arrays, weights):
    _, parts, planes, rows, ny = arrays[0].shape
    nx = 4 * rows
    smem = pl.BlockSpec(memory_space=pltpu.SMEM)
    vmem = pl.BlockSpec(memory_space=pltpu.VMEM)
    return pl.pallas_call(
        functools.partial(lateral_kernel, pieces),
        in_specs=[smem] + [vmem] * (len(arrays) + 2),
        out_specs=[vmem] * 3,
        out_shape=[jax.ShapeDtypeStruct((2, 5, rows, ny), jnp.float32)] * 2
        + [jax.ShapeDtypeStruct(weights.shape + (ny,), jnp.float32)],
        scratch_shapes=[
            pltpu.VMEM((parts, planes, nx, ny), arrays[0].dtype),
            pltpu.VMEM((5, nx, ny), jnp.float32),
        ],
        compiler_params=pltpu.CompilerParams(vmem_limit_bytes=8 << 20),
        name="lateral",
    )(weights, *arrays, stencil(nx).T, stencil(ny))


def ends():
    slab = lax.axis_index("grid")
    levels = lax.axis_size("grid") // 2
    odd = slab % 2
    below = slab // 2
    above = lax.rem(below + 1, levels)
    leave = jnp.where(odd == 1, above, below)
    enter = jnp.where(odd == 1, below, above)
    return any_of(leave, FIRST, levels), any_of(enter, FIRST, levels)


def any_of(cycle, members, levels):
    found = cycle < 0
    for member in members:
        found = found | (cycle == member % levels)
    return found


def places():
    odd = lax.axis_index("grid") % 2
    group = lax.axis_index("band")
    core = group % 2
    half = group // 2
    own = 2 * (1 - odd) + core
    side = 2 * odd + core
    sends, _ = ends()
    quarters = (
        jnp.where(sends, own, side),
        jnp.where(sends, side, own),
        2 * (1 - odd) + 1 - core,
        2 * odd + 1 - core,
    )
    corner = jnp.where(half == odd, 0, 1)
    ahead = corner
    for slab in CELLS:
        at = lax.axis_index("grid") == slab % lax.axis_size("grid")
        ahead = jnp.where(at, 1 - ahead, ahead)
    return quarters + (odd, corner, core, half, ahead, own, side)


def split_kernel(pieces, orbitals, *rest):
    outs, flags, sem = rest[:-2], rest[-2], rest[-1]
    rows = outs[0].shape[3]
    table = places()
    copies = [
        pltpu.make_async_copy(
            orbitals.at[
                low:high, :, :, pl.ds(pl.multiple_of(table[quarter] * rows, rows), rows)
            ],
            out,
            sem.at[i],
        )
        for i, (out, (quarter, low, high)) in enumerate(zip(outs, pieces))
    ]
    for copy in copies:
        copy.start()
    for i, place in enumerate(table):
        flags[i : i + 1] = jnp.full((1, flags.shape[1]), place, jnp.int32)
    for copy in copies:
        copy.wait()


def split(pieces, orbitals):
    _, parts, planes, nx, ny = orbitals.shape
    count = len(pieces)
    return pl.pallas_call(
        functools.partial(split_kernel, pieces),
        in_specs=[pl.BlockSpec(memory_space=pltpu.HBM)],
        out_specs=[pl.BlockSpec(memory_space=pltpu.VMEM)] * (count + 1),
        out_shape=[
            pltpu.VMEM((high - low, parts, planes, nx // 4, ny), orbitals.dtype)
            for _, low, high in pieces
        ]
        + [pltpu.VMEM((16, ny), jnp.int32)],
        scratch_shapes=[pltpu.SemaphoreType.DMA((count,))],
        compiler_params=pltpu.CompilerParams(vmem_limit_bytes=4 << 20),
        name="split",
    )(pltpu.with_memory_space_constraint(orbitals, pltpu.HBM))


def halve_kernel(flags, mine, theirs, kept, sent):
    lower = jnp.broadcast_to(flags[HALF : HALF + 1], kept.shape[1:]) == 0
    for i in range(kept.shape[0]):
        low = mine[0, i] + theirs[0, i]
        high = mine[1, i] + theirs[1, i]
        kept[i] = jnp.where(lower, low, high)
        sent[i] = jnp.where(lower, high, low)


def edges(weights, offset, first, second, sums):
    def advance(n, sums):
        def field(rows, scale=None):
            values = [[rows[n, part, k].astype(jnp.float32) for part in range(2)] for k in range(2)]
            if scale is not None:
                values = [[scale * value for value in plane] for plane in values]
            return values

        def term(low, high):
            return low[0] * high[1] - low[1] * high[0]

        f, g = field(first, weights[pl.ds(n + offset, 1)]), field(second)
        pairs = ((0, 0), (1, 1), (1, 0), (0, 1))
        return tuple(old + term(f[low], g[high]) for old, (low, high) in zip(sums, pairs))

    sums = tuple(sums[i] for i in range(4))
    return lax.fori_loop(0, first.shape[0], advance, sums, unroll=UNROLL)


def flag(flags, which, shape):
    return jnp.broadcast_to(flags[which : which + 1], shape) == 1


def scaled(odd, sums):
    sign = jnp.where(odd, -1.0 / 12.0, 1.0 / 12.0)
    low, high, even_mid, odd_mid = sums
    mid = jnp.where(odd, odd_mid, even_mid)
    up = jnp.where(odd, -8.0 / 12.0, 0.0) * mid
    down = jnp.where(odd, 0.0, 8.0 / 12.0) * mid
    return (up - sign * low, down - sign * high), (down - sign * low, up - sign * high)


def add_edges(weights, offset, own, side, far, inner, outer, before=None):
    zero = (jnp.zeros(inner.shape[1:], jnp.float32),) * 4
    for i, (out, pair) in enumerate(((inner, (own, side)), (outer, (side, far)))):
        start = before[i] if before else zero
        for j, value in enumerate(edges(weights, offset, *pair, start)):
            out[j] = value


def first_kernel(weights, lead, trail, got_lead, got_trail, own1, side1, far1, inner, outer):
    sends, receives = ends()
    for one in (sends, jnp.logical_not(sends)):
        for two in (receives, jnp.logical_not(receives)):
            own = lead if one is sends else trail
            side, far = (got_trail, got_lead) if two is receives else (got_lead, got_trail)
            run = functools.partial(add_edges, weights, 0, own, side, far, inner, outer)
            pl.when(one & two)(run)
    add_edges(weights, lead.shape[0], own1, side1, far1, inner, outer, (inner, outer))


def second_kernel(weights, own, side, far, old_inner, old_outer, inner, outer):
    add_edges(weights, 0, own, side, far, inner, outer, (old_inner, old_outer))


def inner_kernel(offset, flags, weights, own, side, sums, kept, near, inner_side):
    shape = kept.shape[1:]
    odd = flag(flags, ODD, shape)
    here = flag(flags, CORNER, shape)
    own_parts, side_parts = scaled(odd, edges(weights, offset, own, side, sums))
    for plane in range(2):
        kept[plane] = jnp.where(here, own_parts[plane], 0.0)
        near[plane] = jnp.where(here, side_parts[plane], own_parts[plane])
        inner_side[plane] = side_parts[plane]


def outer_kernel(offset, flags, weights, side, far, sums, inner_side, middle, distant):
    shape = middle.shape[1:]
    odd = flag(flags, ODD, shape)
    here = flag(flags, CORNER, shape)
    side_parts, far_parts = scaled(odd, edges(weights, offset, side, far, sums))
    ahead = flag(flags, SWAP, shape)
    for plane in range(2):
        beside = side_parts[plane] + jnp.where(here, 0.0, inner_side[plane])
        middle[plane] = jnp.where(ahead, beside, far_parts[plane])
        distant[plane] = jnp.where(ahead, far_parts[plane], beside)


def call(kernel, arrays, out_shapes):
    vmem = pl.BlockSpec(memory_space=pltpu.VMEM)
    return pl.pallas_call(
        kernel,
        in_specs=[vmem] * len(arrays),
        out_specs=[vmem] * len(out_shapes),
        out_shape=[jax.ShapeDtypeStruct(shape, jnp.float32) for shape in out_shapes],
        compiler_params=pltpu.CompilerParams(vmem_limit_bytes=4 << 20),
    )(*arrays)


def finish_kernel(flat, flat_rest, kept, near, middle, distant, out):
    for plane in range(2):
        parts = kept[plane] + near[plane] + middle[plane] + distant[plane]
        out[0, plane] = flat[0] + flat_rest[0] + parts
        out[1, plane] = flat[1 + plane] + flat_rest[1 + plane]
        out[2, plane] = flat[3 + plane] + flat_rest[3 + plane]


def per_device(orbitals, occupations):
    slabs = lax.axis_size("grid")
    groups = lax.axis_size("band")
    assert groups == 4 and slabs % 2 == 0 and slabs >= 4 and orbitals.shape[2] == 2

    def beyond(g):
        return (g + 2) % slabs if g % 2 else (g - 2) % slabs

    def home(g):
        return (g - 2) % slabs if g % 2 else (g + 2) % slabs

    def route(value, target):
        pairs = []
        for b in range(groups):
            for g in range(slabs):
                goal = target(b, g)
                pairs.append((b * slabs + g, goal[0] * slabs + goal[1]))
        return lax.ppermute(value, ("band", "grid"), pairs)

    bands = orbitals.shape[0]
    cut = bands * 5 // 8
    chunks = ((0, cut), (cut, bands), (0, cut), (cut, bands))
    pieces = [(2 * (k // 2) + part,) + chunk for k, chunk in enumerate(chunks) for part in range(2)]
    lead, trail, flags = split(pieces[:2], orbitals)
    pieces[2:4] = [(OWN, cut, bands), (SIDE, cut, bands)]
    rest = list(split(pieces[2:], orbitals)[:-1])
    arrays = [lead, trail] + rest

    def at_end(g):
        levels = slabs // 2
        return (g // 2 + g % 2) % levels in [member % levels for member in FIRST]

    got_lead = route(lead, lambda b, g: (b, beyond(g) if at_end(g) else g ^ 1))
    got_trail = route(trail, lambda b, g: (b, g ^ 1 if at_end(g) else beyond(g)))
    own, side, far = [None, rest[0], None, None], [None] * 4, [None] * 4
    for k in range(1, 4):
        mine, theirs = rest[2 * k - 2 : 2 * k]
        swap = k // 2
        side[k] = route(theirs, lambda b, g: (b ^ swap, g ^ 1))
        far[k] = route(mine, lambda b, g: (b ^ swap, beyond(g)))
        if swap:
            own[k] = route(mine, lambda b, g: (b ^ 1, g))

    plane = lead.shape[-2:]
    mine, sent, spread = lateral(pieces, arrays, occupations)
    w2 = route(spread, lambda b, g: (b ^ 1, g))
    theirs = route(sent, lambda b, g: (b ^ 1, g))
    flat, sent = call(halve_kernel, (flags, mine, theirs), [(5,) + plane] * 2)
    flat_rest = route(sent, lambda b, g: (b ^ 2, g))

    sums = call(
        first_kernel,
        (spread, lead, trail, got_lead, got_trail, own[1], side[1], far[1]),
        [(4,) + plane] * 2,
    )
    inner, outer = call(second_kernel, (w2, own[2], side[2], far[2], *sums), [(4,) + plane] * 2)
    kept, near, inner_side = call(
        functools.partial(inner_kernel, cut),
        (flags, w2, own[3], side[3], inner),
        [(2,) + plane] * 3,
    )

    def is_corner(b, g):
        return b // 2 != g % 2

    got_near = route(near, lambda b, g: (b, g ^ 1) if is_corner(b, g) else (b ^ 2, g))
    middle, distant = call(
        functools.partial(outer_kernel, cut),
        (flags, w2, side[3], far[3], outer, inner_side),
        [(2,) + plane] * 2,
    )

    def beside(b, g):
        return (b, g ^ 1) if is_corner(b, g) else (b ^ 2, g ^ 1)

    def upward(b, g):
        return (b, home(g)) if is_corner(b, g) else (b ^ 2, home(g))

    def ahead(b, g):
        return is_corner(b, g) != (g in [slab % slabs for slab in CELLS])

    got_middle = route(middle, lambda b, g: beside(b, g) if ahead(b, g) else upward(b, g))
    got_distant = route(distant, lambda b, g: upward(b, g) if ahead(b, g) else beside(b, g))
    arrays = (flat, flat_rest, kept, got_near, got_middle, got_distant)
    (out,) = call(finish_kernel, arrays, [(3, 2) + plane])
    return out


FIRST = (-1,)
CELLS = (1, -1)
UNROLL = 4
FIRST = (-1,)
CELLS = (1, -1)


def solution(mesh):
    placed = (P("band", None, "grid", None, None), P("band"))
    return jax.shard_map(
        per_device,
        mesh=mesh,
        in_specs=placed,
        out_specs=P(None, "grid", "band", None),
        check_vma=False,
    )
```

```python
import functools

import jax
import jax.numpy as jnp
import numpy as np
from jax import lax
from jax.experimental import pallas as pl
from jax.experimental.pallas import tpu as pltpu
from jax.sharding import PartitionSpec as P


ODD, CORNER, CORE, HALF, SWAP, OWN, SIDE, RIDE = range(4, 12)


def stencil(cells):
    eye = np.eye(cells, dtype=np.float32)
    near = np.roll(eye, 1, 0) - np.roll(eye, -1, 0)
    far = np.roll(eye, 2, 0) - np.roll(eye, -2, 0)
    return jnp.asarray(8.0 * near - far, jnp.bfloat16)


def lateral_kernel(pieces, weights, *rest):
    count = len(pieces)
    arrays, (across, along, kept, sent, spread, field, total) = rest[:count], rest[count:]
    _, parts, planes, rows, _ = arrays[0].shape
    bands = max(stop for _, _, stop in pieces)
    table = places()
    total[...] = jnp.zeros_like(total)
    dot = functools.partial(jnp.dot, preferred_element_type=jnp.float32)

    def advance(start, stop, n, carry):
        weight = weights[n]
        for array, (quarter, low, high) in zip(arrays, pieces):
            if low <= start and stop <= high:
                at = pl.ds(pl.multiple_of(table[quarter] * rows, rows), rows)
                for part in range(parts):
                    for plane in range(planes):
                        field[part, plane, at] = array[n - low, part, plane]
        fields = []
        for plane in range(planes):
            re16 = field[0, plane]
            im16 = field[1, plane]
            re = weight * re16.astype(jnp.float32)
            im = weight * im16.astype(jnp.float32)
            fields.append((re, im, re16, im16))
            total[1 + plane] += re * dot(across[...], im16) - im * dot(across[...], re16)
            total[3 + plane] += re * dot(im16, along[...]) - im * dot(re16, along[...])
        (re, im, _, _), (_, _, re_up, im_up) = fields
        total[0] += 8.0 * (re * im_up.astype(jnp.float32) - im * re_up.astype(jnp.float32))
        return carry

    cuts = sorted({cut for _, low, high in pieces for cut in (low, high)})
    for start, stop in zip(cuts, cuts[1:]):
        lax.fori_loop(start, stop, functools.partial(advance, start, stop), 0)
    for n in range(bands):
        spread[n : n + 1] = jnp.full((1, spread.shape[1]), weights[n], jnp.float32)
    core = table[CORE]
    for half in range(2):
        for out, row in ((kept, 2 * half + core), (sent, 2 * half + 1 - core)):
            at = pl.ds(pl.multiple_of(row * rows, rows), rows)
            out[half] = total[:, at] * (1.0 / 12.0)


def lateral(pieces, arrays, weights):
    _, parts, planes, rows, ny = arrays[0].shape
    nx = 4 * rows
    smem = pl.BlockSpec(memory_space=pltpu.SMEM)
    vmem = pl.BlockSpec(memory_space=pltpu.VMEM)
    return pl.pallas_call(
        functools.partial(lateral_kernel, pieces),
        in_specs=[smem] + [vmem] * (len(arrays) + 2),
        out_specs=[vmem] * 3,
        out_shape=[jax.ShapeDtypeStruct((2, 5, rows, ny), jnp.float32)] * 2
        + [jax.ShapeDtypeStruct(weights.shape + (ny,), jnp.float32)],
        scratch_shapes=[
            pltpu.VMEM((parts, planes, nx, ny), arrays[0].dtype),
            pltpu.VMEM((5, nx, ny), jnp.float32),
        ],
        compiler_params=pltpu.CompilerParams(vmem_limit_bytes=8 << 20),
        name="lateral",
    )(weights, *arrays, stencil(nx).T, stencil(ny))


def ends():
    slab = lax.axis_index("grid")
    levels = lax.axis_size("grid") // 2
    odd = slab % 2
    below = slab // 2
    above = lax.rem(below + 1, levels)
    leave = jnp.where(odd == 1, above, below)
    enter = jnp.where(odd == 1, below, above)
    return any_of(leave, FIRST, levels), any_of(enter, FIRST, levels)


def any_of(cycle, members, levels):
    found = cycle < 0
    for member in members:
        found = found | (cycle == member % levels)
    return found


def places():
    odd = lax.axis_index("grid") % 2
    group = lax.axis_index("band")
    core = group % 2
    half = group // 2
    own = 2 * (1 - odd) + core
    side = 2 * odd + core
    sends, _ = ends()
    quarters = (
        jnp.where(sends, own, side),
        jnp.where(sends, side, own),
        2 * (1 - odd) + 1 - core,
        2 * odd + 1 - core,
    )
    corner = jnp.where(half == odd, 0, 1)
    ahead = corner
    for slab in CELLS:
        at = lax.axis_index("grid") == slab % lax.axis_size("grid")
        ahead = jnp.where(at, 1 - ahead, ahead)
    level = lax.axis_index("grid") // 2
    ride = jnp.where((level > 0) & (level < lax.axis_size("grid") // 2 - 1), corner, 0)
    return quarters + (odd, corner, core, half, ahead, own, side, ride)


def split_kernel(pieces, orbitals, *rest):
    outs, flags, sem = rest[:-2], rest[-2], rest[-1]
    rows = outs[0].shape[3]
    table = places()
    copies = [
        pltpu.make_async_copy(
            orbitals.at[
                low:high, :, :, pl.ds(pl.multiple_of(table[quarter] * rows, rows), rows)
            ],
            out,
            sem.at[i],
        )
        for i, (out, (quarter, low, high)) in enumerate(zip(outs, pieces))
    ]
    for copy in copies:
        copy.start()
    for i, place in enumerate(table):
        flags[i : i + 1] = jnp.full((1, flags.shape[1]), place, jnp.int32)
    for copy in copies:
        copy.wait()


def split(pieces, orbitals):
    _, parts, planes, nx, ny = orbitals.shape
    count = len(pieces)
    return pl.pallas_call(
        functools.partial(split_kernel, pieces),
        in_specs=[pl.BlockSpec(memory_space=pltpu.HBM)],
        out_specs=[pl.BlockSpec(memory_space=pltpu.VMEM)] * (count + 1),
        out_shape=[
            pltpu.VMEM((high - low, parts, planes, nx // 4, ny), orbitals.dtype)
            for _, low, high in pieces
        ]
        + [pltpu.VMEM((16, ny), jnp.int32)],
        scratch_shapes=[pltpu.SemaphoreType.DMA((count,))],
        compiler_params=pltpu.CompilerParams(vmem_limit_bytes=4 << 20),
        name="split",
    )(pltpu.with_memory_space_constraint(orbitals, pltpu.HBM))


def halve_kernel(flags, mine, theirs, kept, sent):
    lower = jnp.broadcast_to(flags[HALF : HALF + 1], kept.shape[1:]) == 0
    for i in range(kept.shape[0]):
        low = mine[0, i] + theirs[0, i]
        high = mine[1, i] + theirs[1, i]
        kept[i] = jnp.where(lower, low, high)
        sent[i] = jnp.where(lower, high, low)


def edges(weights, offset, first, second, sums):
    def advance(n, sums):
        def field(rows, scale=None):
            values = [[rows[n, part, k].astype(jnp.float32) for part in range(2)] for k in range(2)]
            if scale is not None:
                values = [[scale * value for value in plane] for plane in values]
            return values

        def term(low, high):
            return low[0] * high[1] - low[1] * high[0]

        f, g = field(first, weights[pl.ds(n + offset, 1)]), field(second)
        pairs = ((0, 0), (1, 1), (1, 0), (0, 1))
        return tuple(old + term(f[low], g[high]) for old, (low, high) in zip(sums, pairs))

    sums = tuple(sums[i] for i in range(4))
    return lax.fori_loop(0, first.shape[0], advance, sums, unroll=UNROLL)


def flag(flags, which, shape):
    return jnp.broadcast_to(flags[which : which + 1], shape) == 1


def scaled(odd, sums):
    sign = jnp.where(odd, -1.0 / 12.0, 1.0 / 12.0)
    low, high, even_mid, odd_mid = sums
    mid = jnp.where(odd, odd_mid, even_mid)
    up = jnp.where(odd, -8.0 / 12.0, 0.0) * mid
    down = jnp.where(odd, 0.0, 8.0 / 12.0) * mid
    return (up - sign * low, down - sign * high), (down - sign * low, up - sign * high)


def add_edges(weights, offset, own, side, far, inner, outer, before=None):
    zero = (jnp.zeros(inner.shape[1:], jnp.float32),) * 4
    for i, (out, pair) in enumerate(((inner, (own, side)), (outer, (side, far)))):
        start = before[i] if before else zero
        for j, value in enumerate(edges(weights, offset, *pair, start)):
            out[j] = value


def first_kernel(weights, lead, trail, got_lead, got_trail, own1, side1, far1, inner, outer):
    sends, receives = ends()
    for one in (sends, jnp.logical_not(sends)):
        for two in (receives, jnp.logical_not(receives)):
            own = lead if one is sends else trail
            side, far = (got_trail, got_lead) if two is receives else (got_lead, got_trail)
            run = functools.partial(add_edges, weights, 0, own, side, far, inner, outer)
            pl.when(one & two)(run)
    add_edges(weights, lead.shape[0], own1, side1, far1, inner, outer, (inner, outer))


def second_kernel(weights, own, side, far, old_inner, old_outer, inner, outer):
    add_edges(weights, 0, own, side, far, inner, outer, (old_inner, old_outer))


def inner_kernel(offset, flags, weights, own, side, sums, kept, near, inner_side):
    shape = kept.shape[1:]
    odd = flag(flags, ODD, shape)
    here = flag(flags, CORNER, shape)
    ride = flag(flags, RIDE, shape)
    own_parts, side_parts = scaled(odd, edges(weights, offset, own, side, sums))
    for plane in range(2):
        kept[plane] = jnp.where(here, own_parts[plane], 0.0)
        part = jnp.where(here, side_parts[plane], own_parts[plane])
        near[plane] = jnp.where(ride, 0.0, part)
        inner_side[plane] = side_parts[plane]


def outer_kernel(offset, flags, weights, side, far, sums, inner_side, middle, distant):
    shape = middle.shape[1:]
    odd = flag(flags, ODD, shape)
    here = flag(flags, CORNER, shape)
    ride = flag(flags, RIDE, shape)
    side_parts, far_parts = scaled(odd, edges(weights, offset, side, far, sums))
    ahead = flag(flags, SWAP, shape)
    for plane in range(2):
        beside = side_parts[plane] + jnp.where(here & ~ride, 0.0, inner_side[plane])
        middle[plane] = jnp.where(ahead, beside, far_parts[plane])
        distant[plane] = jnp.where(ahead, far_parts[plane], beside)


def call(kernel, arrays, out_shapes):
    vmem = pl.BlockSpec(memory_space=pltpu.VMEM)
    return pl.pallas_call(
        kernel,
        in_specs=[vmem] * len(arrays),
        out_specs=[vmem] * len(out_shapes),
        out_shape=[jax.ShapeDtypeStruct(shape, jnp.float32) for shape in out_shapes],
        compiler_params=pltpu.CompilerParams(vmem_limit_bytes=4 << 20),
    )(*arrays)


def finish_kernel(flat, flat_rest, kept, near, middle, distant, out):
    for plane in range(2):
        parts = kept[plane] + near[plane] + middle[plane] + distant[plane]
        out[0, plane] = flat[0] + flat_rest[0] + parts
        out[1, plane] = flat[1 + plane] + flat_rest[1 + plane]
        out[2, plane] = flat[3 + plane] + flat_rest[3 + plane]


def per_device(orbitals, occupations):
    slabs = lax.axis_size("grid")
    groups = lax.axis_size("band")
    assert groups == 4 and slabs % 2 == 0 and slabs >= 4 and orbitals.shape[2] == 2

    def beyond(g):
        return (g + 2) % slabs if g % 2 else (g - 2) % slabs

    def home(g):
        return (g - 2) % slabs if g % 2 else (g + 2) % slabs

    def route(value, target):
        pairs = []
        for b in range(groups):
            for g in range(slabs):
                goal = target(b, g)
                pairs.append((b * slabs + g, goal[0] * slabs + goal[1]))
        return lax.ppermute(value, ("band", "grid"), pairs)

    bands = orbitals.shape[0]
    cut = bands * 5 // 8
    chunks = ((0, cut), (cut, bands), (0, cut), (cut, bands))
    pieces = [(2 * (k // 2) + part,) + chunk for k, chunk in enumerate(chunks) for part in range(2)]
    lead, trail, flags = split(pieces[:2], orbitals)
    pieces[2:4] = [(OWN, cut, bands), (SIDE, cut, bands)]
    rest = list(split(pieces[2:], orbitals)[:-1])
    arrays = [lead, trail] + rest

    def at_end(g):
        levels = slabs // 2
        return (g // 2 + g % 2) % levels in [member % levels for member in FIRST]

    got_lead = route(lead, lambda b, g: (b, beyond(g) if at_end(g) else g ^ 1))
    got_trail = route(trail, lambda b, g: (b, g ^ 1 if at_end(g) else beyond(g)))
    own, side, far = [None, rest[0], None, None], [None] * 4, [None] * 4
    for k in range(1, 4):
        mine, theirs = rest[2 * k - 2 : 2 * k]
        swap = k // 2
        side[k] = route(theirs, lambda b, g: (b ^ swap, g ^ 1))
        far[k] = route(mine, lambda b, g: (b ^ swap, beyond(g)))
        if swap:
            own[k] = route(mine, lambda b, g: (b ^ 1, g))

    plane = lead.shape[-2:]
    mine, sent, spread = lateral(pieces, arrays, occupations)
    w2 = route(spread, lambda b, g: (b ^ 1, g))
    theirs = route(sent, lambda b, g: (b ^ 1, g))
    flat, sent = call(halve_kernel, (flags, mine, theirs), [(5,) + plane] * 2)
    flat_rest = route(sent, lambda b, g: (b ^ 2, g))

    sums = call(
        first_kernel,
        (spread, lead, trail, got_lead, got_trail, own[1], side[1], far[1]),
        [(4,) + plane] * 2,
    )
    inner, outer = call(second_kernel, (w2, own[2], side[2], far[2], *sums), [(4,) + plane] * 2)
    kept, near, inner_side = call(
        functools.partial(inner_kernel, cut),
        (flags, w2, own[3], side[3], inner),
        [(2,) + plane] * 3,
    )

    def is_corner(b, g):
        return b // 2 != g % 2

    def near_goal(b, g):
        inside_z = 0 < g // 2 < slabs // 2 - 1
        return (b, g ^ 1) if is_corner(b, g) and not inside_z else (b ^ 2, g)

    got_near = route(near, near_goal)
    middle, distant = call(
        functools.partial(outer_kernel, cut),
        (flags, w2, side[3], far[3], outer, inner_side),
        [(2,) + plane] * 2,
    )

    def beside(b, g):
        return (b, g ^ 1) if is_corner(b, g) else (b ^ 2, g ^ 1)

    def upward(b, g):
        return (b, home(g)) if is_corner(b, g) else (b ^ 2, home(g))

    def ahead(b, g):
        return is_corner(b, g) != (g in [slab % slabs for slab in CELLS])

    got_middle = route(middle, lambda b, g: beside(b, g) if ahead(b, g) else upward(b, g))
    got_distant = route(distant, lambda b, g: upward(b, g) if ahead(b, g) else beside(b, g))
    arrays = (flat, flat_rest, kept, got_near, got_middle, got_distant)
    (out,) = call(finish_kernel, arrays, [(3, 2) + plane])
    return out


FIRST = (-1,)
CELLS = (1, 5, -1)
UNROLL = 4
FIRST = (-1,)
CELLS = (1, 5, -1)


def solution(mesh):
    placed = (P("band", None, "grid", None, None), P("band"))
    return jax.shard_map(
        per_device,
        mesh=mesh,
        in_specs=placed,
        out_specs=P(None, "grid", "band", None),
        check_vma=False,
    )
```
